32 devices in a mesh: rep: 4 (over y, z), data: 8 (over x, core).
Axes of the slice: x: 4, y: 2, z: 2, core: 2. Of those that a mesh axis runs over, the one named last changes fastest.
The devices are a block of a 4x4x8 slice.
Arguments:
- x: bfloat16 [2048, 2048], P(('rep', 'data')), parts along dimension 0
- adapter_id: int32 [2048], P(('rep', 'data')), parts along dimension 0
- w_gate: bfloat16 [2048, 5632], replicated
- w_up: bfloat16 [2048, 5632], replicated
- w_down: bfloat16 [5632, 2048], replicated
- a_gate: bfloat16 [1024, 8, 2048], P('data')
- b_gate: bfloat16 [1024, 8, 5632], P('data')
- a_up: bfloat16 [1024, 8, 2048], P('data')
- b_up: bfloat16 [1024, 8, 5632], P('data')
- a_down: bfloat16 [1024, 8, 5632], P('data')
- b_down: bfloat16 [1024, 8, 2048], P('data')
Outputs:
- output: bfloat16 [2048, 2048], P(('rep', 'data')), parts along dimension 0
There are 4 independent parts. The reference program is written for one: setup_inputs(seed, part) draws one part's arguments, and reference() takes and returns one part's arrays. A program takes and returns all parts, laid end to end along the dimension named above; an argument that names none is the same for every part.
All inputs are finite; a program needn't handle non-finite values.
Results may differ from the reference program's by a relative error of at most 0.00571596.
Values are sent between devices in bfloat16 or wider.
A program may use at most 768 MiB of HBM per device.

```python
import jax
import jax.numpy as jnp
from jax import lax

D = 2048
FF = 5632
RANK = 8
ADAPTERS = 1024
TOK = 64
GROUP = 8
CAP = 24
LORA_ALPHA = 32

SCALE = LORA_ALPHA / RANK
TOKENS = TOK * GROUP
PER_OWNER = ADAPTERS // GROUP


def shuffle_row(row_key, row_owner):
    return row_owner[jax.random.permutation(row_key, TOK)]


def draw_ids(id_key):
    id_keys = jax.random.split(id_key, 5)
    hot_owner = jax.random.randint(id_keys[0], (), 0, GROUP)
    offset = jax.random.randint(id_keys[1], (), 0, GROUP - 1)
    source = jnp.arange(GROUP)[:, None]
    position = jnp.arange(TOK)[None, :]
    spread = (offset + source * (TOK - CAP) + position - CAP) % (GROUP - 1)
    owner_idx = jnp.where(position < CAP, hot_owner, (hot_owner + 1 + spread) % GROUP)
    owner_idx = jax.vmap(shuffle_row)(jax.random.split(id_keys[2], GROUP), owner_idx)
    flat_owner = owner_idx.reshape(TOKENS)
    owner_hot = (flat_owner[:, None] == jnp.arange(GROUP)[None, :]).astype(jnp.int32)
    arrival = jnp.sum(jnp.cumsum(owner_hot, axis=0) * owner_hot, axis=1) - 1
    popular = jnp.minimum(jax.random.randint(id_keys[3], (TOKENS,), 0, PER_OWNER), jax.random.randint(id_keys[4], (TOKENS,), 0, PER_OWNER))
    local_idx = jnp.where(arrival == 0, 0, jnp.where(arrival == 1, PER_OWNER - 1, popular))
    return (flat_owner * PER_OWNER + local_idx).astype(jnp.int32)


def setup_inputs(seed: int = 0, part: int = 0) -> dict:
    key = jax.random.key(seed)
    weight_keys = jax.random.split(key, 9)
    part_keys = jax.random.split(jax.random.fold_in(key, part), 2)
    b_scale = 0.3 / (SCALE * RANK ** 0.5)

    def draw_normal(index, shape, std):
        return (jax.random.normal(weight_keys[index], shape, jnp.float32) * std).astype(jnp.bfloat16)

    return {
        "x": jax.random.normal(part_keys[0], (TOKENS, D), jnp.float32).astype(jnp.bfloat16),
        "adapter_id": draw_ids(part_keys[1]),
        "w_gate": draw_normal(0, (D, FF), D ** -0.5),
        "w_up": draw_normal(1, (D, FF), D ** -0.5),
        "w_down": draw_normal(2, (FF, D), FF ** -0.5),
        "a_gate": draw_normal(3, (ADAPTERS, RANK, D), D ** -0.5),
        "b_gate": draw_normal(4, (ADAPTERS, RANK, FF), b_scale),
        "a_up": draw_normal(5, (ADAPTERS, RANK, D), D ** -0.5),
        "b_up": draw_normal(6, (ADAPTERS, RANK, FF), b_scale),
        "a_down": draw_normal(7, (ADAPTERS, RANK, FF), FF ** -0.5),
        "b_down": draw_normal(8, (ADAPTERS, RANK, D), b_scale),
    }


def lora_delta(tok_rows, tok_ids, a_mat, b_mat):
    a_rows = a_mat[tok_ids].astype(jnp.float32)
    b_rows = b_mat[tok_ids].astype(jnp.float32)
    low_rank = jnp.einsum("td,trd->tr", tok_rows.astype(jnp.float32), a_rows).astype(jnp.bfloat16)
    full_rows = jnp.einsum("tr,trf->tf", low_rank.astype(jnp.float32), b_rows)
    return (SCALE * full_rows).astype(jnp.bfloat16)


def reference(x, adapter_id, w_gate, w_up, w_down, a_gate, b_gate, a_up, b_up, a_down, b_down):
    def one_block(block_in):
        tok_rows, tok_ids = block_in
        gate_pre = jnp.dot(tok_rows, w_gate, preferred_element_type=jnp.float32) + lora_delta(tok_rows, tok_ids, a_gate, b_gate).astype(jnp.float32)
        up_pre = jnp.dot(tok_rows, w_up, preferred_element_type=jnp.float32) + lora_delta(tok_rows, tok_ids, a_up, b_up).astype(jnp.float32)
        hidden = (jax.nn.silu(gate_pre) * up_pre).astype(jnp.bfloat16)
        down_out = jnp.dot(hidden, w_down, preferred_element_type=jnp.float32) + lora_delta(hidden, tok_ids, a_down, b_down).astype(jnp.float32)
        return (tok_rows.astype(jnp.float32) + down_out).astype(jnp.bfloat16)

    blocks = (x.reshape(GROUP, TOK, D), adapter_id.reshape(GROUP, TOK))
    return lax.map(one_block, blocks).reshape(TOKENS, D)
```

```python
import functools

import jax
import jax.numpy as jnp
from jax import lax
from jax.experimental import pallas as pl
from jax.experimental.pallas import tpu as pltpu
from jax.sharding import PartitionSpec as P

LORA_ALPHA = 32
F32 = jnp.float32
BF16 = jnp.bfloat16
MESH = pl.DeviceIdType.MESH

KC = 512
FT = 512
NT = 256
W_SLOTS = 3
S_SLOTS = 12
D_SLOTS = 4


def nt_dot(a, b):
    return lax.dot_general(a, b, (((1,), (1,)), ((), ())), preferred_element_type=F32)


def kernel(groups, scale, rank, ids_ref, x_ref, wg, wu, wd, ag, au, ad, bg, bu, bd, out_ref,
           wbuf, sbuf, dbuf, acc, low, lowm, lowd, xs, hid,
           xsend, xrecv, lsend, lrecv, osend, orecv,
           wsem, ssem, dsem, xs_sem, xr_sem, ls_sem, lr_sem, os_sem, or_sem):
    me = lax.axis_index("data")
    tok, d = x_ref.shape
    ff = wd.shape[0]
    na = ag.shape[0]
    per_owner = na // rank
    cap = xsend.shape[2]
    rows = groups * cap
    nq, nf, nn = d // KC, ff // FT, d // NT
    nw = 2 * nq

    barrier = pltpu.get_barrier_semaphore()
    for j in range(1, groups):
        pl.semaphore_signal(barrier, inc=1, device_id={"data": lax.rem(me + j, groups)}, device_id_type=MESH)

    def w_copy(i, p, q):
        src = (wg, wu)[p]
        slot = lax.rem(i, W_SLOTS)
        return pltpu.make_async_copy(src.at[pl.ds(q * KC, KC), :], wbuf.at[slot], wsem.at[slot])

    def s_copy_a(p, q):
        slot = 2 * q + p
        return pltpu.make_async_copy((ag, au)[p].at[:, pl.ds(q * KC, KC)], sbuf.at[slot], ssem.at[slot])

    def s_copy_f(t, f):
        slot = lax.rem(2 * nq + 3 * f + t, S_SLOTS)
        return pltpu.make_async_copy((bg, bu, ad)[t].at[:, pl.ds(f * FT, FT)], sbuf.at[slot], ssem.at[slot])

    def s_copy_b(m):
        slot = lax.rem(2 * nq + 3 * nf + m, S_SLOTS)
        return pltpu.make_async_copy(bd.at[:, pl.ds(m * FT, FT)], sbuf.at[slot], ssem.at[slot])

    nb = d // FT

    def s_issue(b):
        k = b - 2 * nq
        for t in range(3):
            @pl.when(jnp.logical_and(k < 3 * nf, lax.rem(k, 3) == t))
            def _():
                s_copy_f(t, k // 3).start()

        @pl.when(jnp.logical_and(k >= 3 * nf, k < 3 * nf + nb))
        def _():
            s_copy_b(k - 3 * nf).start()

    def d_copy(n):
        slot = lax.rem(n, D_SLOTS)
        return pltpu.make_async_copy(wd.at[:, pl.ds(n * NT, NT)], dbuf.at[slot], dsem.at[slot])

    for q in range(nq):
        for p in range(2):
            s_copy_a(p, q).start()
            if 2 * q + p < W_SLOTS:
                w_copy(2 * q + p, p, q).start()
    for b in range(2 * nq, S_SLOTS):
        s_copy_f((b - 2 * nq) % 3, (b - 2 * nq) // 3).start()

    ids_row = ids_ref[...]
    own_row = ids_row // per_owner
    ti = lax.broadcasted_iota(jnp.int32, (tok, tok), 0)
    tj = lax.broadcasted_iota(jnp.int32, (tok, tok), 1)
    eye = ti == tj
    ids_col = jnp.sum(jnp.where(eye, ids_row, 0), axis=1, keepdims=True)
    own_col = ids_col // per_owner
    same = own_col == own_row
    arr_row = jnp.sum(jnp.where(jnp.logical_and(same, ti < tj), 1, 0), axis=0, keepdims=True)
    arr_col = jnp.sum(jnp.where(jnp.logical_and(same, tj < ti), 1, 0), axis=1, keepdims=True)
    slot_row = own_row * cap + arr_row
    slot_col = own_col * cap + arr_col
    pick = (lax.broadcasted_iota(jnp.int32, (rows, tok), 0) == slot_row).astype(F32).astype(BF16)
    back = (lax.broadcasted_iota(jnp.int32, (tok, rows), 1) == slot_col).astype(F32).astype(BF16)
    loc = jnp.broadcast_to((ids_col - own_col * per_owner).astype(F32), (tok, 128)).astype(BF16)
    lsend[...] = jnp.dot(pick, loc, preferred_element_type=F32).reshape(groups, cap, 128).astype(BF16)
    for q in range(nq):
        part = jnp.dot(pick, x_ref[:, q * KC:(q + 1) * KC], preferred_element_type=F32)
        xsend[q] = part.reshape(groups, cap, KC).astype(BF16)

    pl.semaphore_wait(barrier, groups - 1)

    def l_copy(j):
        to = lax.rem(me + j, groups)
        return pltpu.make_async_remote_copy(lsend.at[to], lrecv.at[me], ls_sem.at[j], lr_sem.at[j], device_id={"data": to}, device_id_type=MESH)

    def x_copy(q, j):
        to = lax.rem(me + j, groups)
        return pltpu.make_async_remote_copy(xsend.at[q, to], xrecv.at[q, me], xs_sem.at[q, j], xr_sem.at[q, j], device_id={"data": to}, device_id_type=MESH)

    def o_copy(n, j):
        to = lax.rem(me + j, groups)
        return pltpu.make_async_remote_copy(osend.at[n, to], orecv.at[n, me], os_sem.at[n, j], or_sem.at[n, j], device_id={"data": to}, device_id_type=MESH)

    for j in range(1, groups):
        l_copy(j).start()
    for q in range(nq):
        for j in range(1, groups):
            x_copy(q, j).start()
    lrecv[me] = lsend[me]
    for q in range(nq):
        xrecv[q, me] = xsend[q, me]

    low[...] = jnp.zeros_like(low)
    acc[...] = jnp.zeros_like(acc)
    lowd[...] = jnp.zeros_like(lowd)

    def k_step(q, carry):
        for j in range(1, groups):
            x_copy(q, j).wait_recv()
        xq = xrecv[q].astype(F32).reshape(rows, KC).astype(BF16)
        xs[q] = xq
        for p in range(2):
            i = 2 * q + p
            slot = lax.rem(i, W_SLOTS)
            s_copy_a(p, q).wait()
            low[p] += nt_dot(xq, sbuf[i])
            s_issue(i + S_SLOTS)
            w_copy(i, p, q).wait()
            for n in range(nf):
                cols = slice(n * FT, (n + 1) * FT)
                acc[p, :, cols] += jnp.dot(xq, wbuf[slot, :, cols], preferred_element_type=F32)
            nxt = i + W_SLOTS
            pn = (p + W_SLOTS) % 2

            @pl.when(nxt < nw)
            def _():
                w_copy(nxt, pn, nxt // 2).start()
        return carry

    lax.fori_loop(0, nq, k_step, 0)

    for j in range(1, groups):
        l_copy(j).wait_recv()
    loc_in = lrecv[...].astype(F32).reshape(rows, 128)
    lane_ad = (lax.broadcasted_iota(jnp.int32, (rows, 128), 1) // rank).astype(F32)

    def keep_own(v):
        parts = []
        for c in range(na // 128):
            own = loc_in == lane_ad + float(c * (128 // rank))
            parts.append(jnp.where(own, v[:, c * 128:(c + 1) * 128], 0.0).astype(BF16))
        return jnp.concatenate(parts, axis=1)

    for p in range(2):
        lowm[p] = keep_own(low[p])

    def f_step(f, carry):
        pre = []
        cols = pl.ds(pl.multiple_of(f * FT, FT), FT)
        for p in range(2):
            s_copy_f(p, f).wait()
            b = 2 * nq + 3 * f + p
            slot = lax.rem(b, S_SLOTS)
            delta = (scale * jnp.dot(lowm[p], sbuf[slot], preferred_element_type=F32)).astype(BF16)
            pre.append(acc[p, :, cols] + delta.astype(F32))
            s_issue(b + S_SLOTS)
        h = (jax.nn.silu(pre[0]) * pre[1]).astype(BF16)
        hid[:, cols] = h
        s_copy_f(2, f).wait()
        b = 2 * nq + 3 * f + 2
        lowd[...] += nt_dot(h, sbuf[lax.rem(b, S_SLOTS)])
        s_issue(b + S_SLOTS)

        @pl.when(jnp.logical_and(lax.rem(f, 2) == 0, f // 2 < D_SLOTS))
        def _():
            d_copy(f // 2).start()
        return carry

    lax.fori_loop(0, nf, f_step, 0)
    lowm[0] = keep_own(lowd[...])

    per_b = FT // NT

    def n_step(n, carry):
        m = n // per_b
        slot = lax.rem(2 * nq + 3 * nf + m, S_SLOTS)

        @pl.when(lax.rem(n, per_b) == 0)
        def _():
            s_copy_b(m).wait()
        bcols = pl.ds(pl.multiple_of(lax.rem(n, per_b) * NT, NT), NT)
        delta = (scale * jnp.dot(lowm[0], sbuf[slot, :, bcols], preferred_element_type=F32)).astype(BF16)
        d_copy(n).wait()
        ds = lax.rem(n, D_SLOTS)
        base = jnp.dot(hid[...], dbuf[ds], preferred_element_type=F32)
        xcols = pl.ds(pl.multiple_of(lax.rem(n, KC // NT) * NT, NT), NT)
        res = xs[n // (KC // NT), :, xcols].astype(F32) + (base + delta.astype(F32))
        osend[n] = res.reshape(groups, cap, NT).astype(BF16)
        for j in range(1, groups):
            o_copy(n, j).start()

        @pl.when(n + D_SLOTS < nn)
        def _():
            d_copy(n + D_SLOTS).start()
        orecv[n, me] = osend[n, me]
        return carry

    lax.fori_loop(0, nn, n_step, 0)

    for n in range(nn):
        for j in range(1, groups):
            o_copy(n, j).wait_recv()
        got = orecv[n].astype(F32).reshape(rows, NT).astype(BF16)
        out_ref[:, n * NT:(n + 1) * NT] = jnp.dot(back, got, preferred_element_type=F32).astype(BF16)

    for j in range(1, groups):
        l_copy(j).wait_send()
        for q in range(nq):
            x_copy(q, j).wait_send()
        for n in range(nn):
            o_copy(n, j).wait_send()


def solution(mesh):
    groups = mesh.shape["data"]
    row_spec = P(("rep", "data"), None)
    id_spec = P(("rep", "data"))
    owned_spec = P("data", None, None)

    def device_step(x, adapter_id, w_gate, w_up, w_down, a_gate, b_gate, a_up, b_up, a_down, b_down):
        tok, d = x.shape
        ff = w_gate.shape[1]
        per_owner, rank = a_gate.shape[:2]
        na = per_owner * rank
        cap = (3 * tok + groups - 1) // groups
        rows = groups * cap
        nq, nn = d // KC, d // NT

        def flat(a):
            return a.reshape(na, a.shape[2])

        hbm = pl.BlockSpec(memory_space=pl.ANY)
        vmem = pl.BlockSpec(memory_space=pltpu.VMEM)
        dma = pltpu.SemaphoreType.DMA
        return pl.pallas_call(
            functools.partial(kernel, groups, LORA_ALPHA / rank, rank),
            out_shape=jax.ShapeDtypeStruct((tok, d), BF16),
            in_specs=[vmem, vmem] + [hbm] * 9,
            out_specs=vmem,
            scratch_shapes=[
                pltpu.VMEM((W_SLOTS, KC, ff), BF16),
                pltpu.VMEM((S_SLOTS, na, FT), BF16),
                pltpu.VMEM((D_SLOTS, ff, NT), BF16),
                pltpu.VMEM((2, rows, ff), F32),
                pltpu.VMEM((2, rows, na), F32),
                pltpu.VMEM((2, rows, na), BF16),
                pltpu.VMEM((rows, na), F32),
                pltpu.VMEM((nq, rows, KC), BF16),
                pltpu.VMEM((rows, ff), BF16),
                pltpu.VMEM((nq, groups, cap, KC), BF16),
                pltpu.VMEM((nq, groups, cap, KC), BF16),
                pltpu.VMEM((groups, cap, 128), BF16),
                pltpu.VMEM((groups, cap, 128), BF16),
                pltpu.VMEM((nn, groups, cap, NT), BF16),
                pltpu.VMEM((nn, groups, cap, NT), BF16),
                dma((W_SLOTS,)), dma((S_SLOTS,)), dma((D_SLOTS,)),
                dma((nq, groups)), dma((nq, groups)),
                dma((groups,)), dma((groups,)),
                dma((nn, groups)), dma((nn, groups)),
            ],
            compiler_params=pltpu.CompilerParams(collective_id=0, has_side_effects=True, vmem_limit_bytes=67043328),
            name="lora_layer",
        )(adapter_id.reshape(1, tok), x, w_gate, w_up, w_down, flat(a_gate), flat(a_up), flat(a_down), flat(b_gate), flat(b_up), flat(b_down))

    return jax.shard_map(device_step, mesh=mesh, in_specs=(row_spec, id_spec, P(), P(), P(), owned_spec, owned_spec, owned_spec, owned_spec, owned_spec, owned_spec), out_specs=row_spec, check_vma=False)
```

```python
import functools

import jax
import jax.numpy as jnp
from jax import lax
from jax.experimental import pallas as pl
from jax.experimental.pallas import tpu as pltpu
from jax.sharding import PartitionSpec as P

LORA_ALPHA = 32
F32 = jnp.float32
BF16 = jnp.bfloat16
MESH = pl.DeviceIdType.MESH

KB = 512
VMEM_LIMIT = 67043328


def nt_dot(a, b):
    return lax.dot_general(a, b, (((1,), (1,)), ((), ())), preferred_element_type=F32)


def kernel(groups, scale, rank, ids_hbm, x_hbm, wg, wu, wd, ag, au, ad, bg, bu, bd, out_ref,
           ids_ref, x_ref, pool, acc, low, lowd, lowm, xs, hid, xsend, xrecv, lsend, lrecv, osend, orecv,
           w_sem, g_sem, in_sem, xs_sem, xr_sem, ls_sem, lr_sem, os_sem, or_sem):
    me = lax.axis_index("data")
    partner = me + 1 - 2 * lax.rem(me, 2)
    tok, d = x_hbm.shape
    nf, ra = wd.shape[0], ag.shape[0]
    na = ra * KB
    per_owner = na // rank
    cap = xsend.shape[2]
    rows = groups * cap
    slots = pool.shape[0]
    nq = nm = d // KB

    peers = [lax.rem(base + 4, groups) for base in (me, partner)]
    peers += [lax.rem(me + 2, groups), lax.rem(me + 6, groups), lax.rem(partner + 2, groups), lax.rem(partner + 6, groups), partner]
    assert groups == 8
    links = range(groups - 1)

    barrier = pltpu.get_barrier_semaphore()
    for to in peers:
        pl.semaphore_signal(barrier, inc=1, device_id={"data": to}, device_id_type=MESH)
    ids_copy = pltpu.make_async_copy(ids_hbm, ids_ref, in_sem.at[0])
    x_in = pltpu.make_async_copy(x_hbm, x_ref, in_sem.at[1])
    ids_copy.start()
    x_in.start()

    per_k = 2 * (nf + ra)
    per_f = 3 * ra
    per_m = nf + ra
    f_base = nq * per_k
    per_b = 2 * ra
    m_base = f_base + nf * per_f
    d_base = m_base + nm * ra
    total = d_base + nm * nf

    def slot_of(i):
        return i % slots if isinstance(i, int) else lax.rem(i, slots)

    ring = slots // per_k
    assert slots % per_k == 0

    def w_block(q, p, n):
        s = slot_of(q * per_k + p * nf + n)
        return pltpu.make_async_copy((wg, wu)[p].at[pl.ds(q * KB, KB), pl.ds(n * KB, KB)], pool.at[s], w_sem.at[q % ring if isinstance(q, int) else lax.rem(q, ring)])

    def w_wait(q):
        s = slot_of(q * per_k)
        every = pool.at[pl.ds(s, 2 * nf)]
        pltpu.make_async_copy(every, every, w_sem.at[q % ring if isinstance(q, int) else lax.rem(q, ring)]).wait()

    def group(src, c, i):
        count = src.shape[0]
        s = slot_of(i)
        if isinstance(s, int):
            assert s + count <= slots
        return pltpu.make_async_copy(src.at[:, :, pl.ds(c * KB, KB)], pool.at[pl.ds(s, count)], g_sem.at[s])

    def a_group(q, p):
        return group((ag, au)[p], q, q * per_k + 2 * nf + p * ra)

    def b_at(f, p):
        return f_base + (p * ra if isinstance(f, int) and f == 0 else f * per_f - ra + p * ra)

    def b_group(f, p):
        return group((bg, bu)[p], f, b_at(f, p))

    def ad_at(f):
        return m_base - ra if isinstance(f, int) and f == nf - 1 else f_base + (f + 1) * per_f + per_b - ra

    def ad_group(f):
        return group(ad, f, ad_at(f))

    def bd_group(m):
        return group(bd, m, m_base + m * ra)

    def wd_group(m):
        return group(wd, m, d_base + m * nf)

    later = [(b_at(f, p), ra, b_group(f, p)) for f in range(nf) for p in range(2)]
    later += [(ad_at(f), ra, ad_group(f)) for f in range(nf)]
    later += [(m_base + m * ra, ra, bd_group(m)) for m in range(nm)]
    later += [(d_base + m * nf, nf, wd_group(m)) for m in range(nm)]
    later.sort(key=lambda t: t[0])
    assert [t[0] for t in later] == [f_base + sum(t[1] for t in later[:k]) for k in range(len(later))]

    def k_start(q):
        for p in range(2):
            for n in range(nf):
                w_block(q, p, n).start()
            a_group(q, p).start()

    def start_between(lo, hi):
        for i, count, copy in later:
            if lo <= i + count - 1 - slots < hi:
                copy.start()

    k_start(0)

    ids_copy.wait()
    ids_row = ids_ref[...]
    own_row = ids_row // per_owner
    ti = lax.broadcasted_iota(jnp.int32, (tok, tok), 0)
    tj = lax.broadcasted_iota(jnp.int32, (tok, tok), 1)
    eye = ti == tj
    ids_col = jnp.sum(jnp.where(eye, ids_row, 0), axis=1, keepdims=True)
    own_col = ids_col // per_owner
    same = own_col == own_row
    arr_row = jnp.sum(jnp.where(jnp.logical_and(same, ti < tj), 1, 0), axis=0, keepdims=True)
    arr_col = jnp.sum(jnp.where(jnp.logical_and(same, tj < ti), 1, 0), axis=1, keepdims=True)
    slot_row = own_row * cap + arr_row
    slot_col = own_col * cap + arr_col
    pick = (lax.broadcasted_iota(jnp.int32, (rows, tok), 0) == slot_row).astype(F32).astype(BF16)
    back = (lax.broadcasted_iota(jnp.int32, (tok, rows), 1) == slot_col).astype(F32).astype(BF16)
    loc = jnp.broadcast_to((ids_col - own_col * per_owner).astype(F32), (tok, 128)).astype(BF16)
    lsend[...] = jnp.dot(pick, loc, preferred_element_type=F32).reshape(groups, cap, 128).astype(BF16)
    x_in.wait()
    for q in range(nq):
        part = jnp.dot(pick, x_ref[:, q * KB:(q + 1) * KB], preferred_element_type=F32)
        xsend[q] = part.reshape(groups, cap, KB).astype(BF16)

    pl.semaphore_wait(barrier, groups - 1)

    def remote(src, dst, j, send_sem, recv_sem):
        return pltpu.make_async_remote_copy(src.at[peers[j]], dst.at[me], send_sem.at[j], recv_sem.at[j], device_id={"data": peers[j]}, device_id_type=MESH)

    def l_copy(j):
        return remote(lsend, lrecv, j, ls_sem, lr_sem)

    def x_copy(q, j):
        return remote(xsend.at[q], xrecv.at[q], j, xs_sem.at[q], xr_sem.at[q])

    def o_copy(m, j):
        return remote(osend.at[m], orecv.at[m], j, os_sem.at[m], or_sem.at[m])

    for q in range(nq):
        for j in links:
            x_copy(q, j).start()
    for j in links:
        l_copy(j).start()
    for q in range(1, ring):
        k_start(q)
    lrecv[me] = lsend[me]
    for q in range(nq):
        xrecv[q, me] = xsend[q, me]

    low[...] = jnp.zeros_like(low)
    acc[...] = jnp.zeros_like(acc)
    lowd[...] = jnp.zeros_like(lowd)

    def k_in(q):
        for j in links:
            x_copy(q, j).wait_recv()
        xq = xrecv[q].astype(F32).reshape(rows, KB).astype(BF16)
        xs[q] = xq
        for p in range(2):
            a_group(q, p).wait()
        w_wait(q)
        return xq

    def k_low(q, xq):
        for p in range(2):
            for r in range(ra):
                low[p, r] += nt_dot(pool[slot_of(q * per_k + 2 * nf + p * ra) + r], xq)

    def k_base(q, xq):
        s0 = slot_of(q * per_k)
        for p in range(2):
            for n in range(nf):
                acc[p, n] += jnp.dot(xq, pool[s0 + p * nf + n], preferred_element_type=F32)

    def k_step(q, carry):
        xq = k_in(q)
        k_low(q, xq)
        k_base(q, xq)
        for z in range(nq - 1):
            @pl.when(q == z)
            def _():
                if z + ring < nq:
                    k_start(z + ring)
                start_between(z * per_k, (z + 1) * per_k)
        return carry

    lax.fori_loop(0, nq - 1, k_step, 0)

    xq = k_in(nq - 1)
    for j in links:
        l_copy(j).wait_recv()
    loc_in = lrecv[...].astype(F32).reshape(rows, 128).astype(BF16)
    lane0 = (lax.broadcasted_iota(jnp.int32, (8, 128), 1) == 0).astype(F32).astype(BF16)
    loc_row = nt_dot(lane0, loc_in)[0:1, :]
    ad_col = (lax.broadcasted_iota(jnp.int32, (KB, rows), 0) // rank).astype(F32)
    unit = (lax.broadcasted_iota(jnp.int32, (rows, rows), 0) == lax.broadcasted_iota(jnp.int32, (rows, rows), 1)).astype(F32).astype(BF16)

    def keep_own(v, r):
        own = ad_col + float(r * (KB // rank)) == loc_row
        kept = jnp.where(own, v, 0.0).astype(BF16)
        return nt_dot(unit, kept).astype(BF16)

    k_low(nq - 1, xq)
    for p in range(2):
        for r in range(ra):
            lowm[p, r] = keep_own(low[p, r], r)
    k_base(nq - 1, xq)
    start_between((nq - 1) * per_k, nq * per_k)
    for j in links:
        l_copy(j).wait_send()
        for q in range(nq):
            x_copy(q, j).wait_send()

    def low_dot(p, i0):
        full = jnp.dot(lowm[p, 0], pool[slot_of(i0)], preferred_element_type=F32)
        for r in range(1, ra):
            full += jnp.dot(lowm[p, r], pool[slot_of(i0) + r], preferred_element_type=F32)
        return (scale * full).astype(BF16).astype(F32)

    def hidden(f):
        g = acc[0, f] + low_dot(0, b_at(f, 0))
        u = acc[1, f] + low_dot(1, b_at(f, 1))
        return (jax.nn.silu(g) * u).astype(BF16)

    def low_down(f):
        for r in range(ra):
            lowd[r] += nt_dot(pool[slot_of(ad_at(f)) + r], hid[f])

    for p in range(2):
        b_group(0, p).wait()
    hid[0] = hidden(0)
    start_between(f_base, f_base + per_b)

    def f_step(g, carry):
        steps = [pair * g + 1 + z for z in range(pair)]
        for f in steps:
            for p in range(2):
                b_group(f, p).wait()
            ad_group(f - 1).wait()
        for f in steps:
            h = hidden(f)
            low_down(f - 1)
            hid[f] = h
        for z in range((nf - 1) // pair):
            @pl.when(g == z)
            def _():
                lo = f_base + per_b + z * pair * per_f
                start_between(lo, lo + pair * per_f)
        return carry

    pair = 2 if nf % 2 == 1 else 1
    lax.fori_loop(0, (nf - 1) // pair, f_step, 0)
    assert m_base - ra + slots >= total

    def m_in(m):
        bd_group(m).wait()
        wd_group(m).wait()

    def m_base_dot(m):
        s0 = slot_of(d_base + m * nf)
        base = jnp.dot(hid[0], pool[s0], preferred_element_type=F32)
        for k in range(1, nf):
            base += jnp.dot(hid[k], pool[s0 + k], preferred_element_type=F32)
        return base

    def m_out(m, base):
        res = xs[m].astype(F32) + (base + low_dot(0, m_base + m * ra))
        osend[m] = res.reshape(groups, cap, KB).astype(BF16)
        for j in links:
            o_copy(m, j).start()
        orecv[m, me] = osend[m, me]

    ad_group(nf - 1).wait()
    m_in(0)
    low_down(nf - 1)
    base = m_base_dot(0)
    for r in range(ra):
        lowm[0, r] = keep_own(lowd[r], r)
    m_out(0, base)

    def m_step(m, carry):
        m_in(m)
        m_out(m, m_base_dot(m))
        return carry

    lax.fori_loop(1, nm, m_step, 0)

    for m in range(nm):
        for j in links:
            o_copy(m, j).wait_recv()
            o_copy(m, j).wait_send()
        got = orecv[m].astype(F32).reshape(rows, KB).astype(BF16)
        out_ref[:, m * KB:(m + 1) * KB] = jnp.dot(back, got, preferred_element_type=F32).astype(BF16)


def solution(mesh):
    groups = mesh.shape["data"]
    row_spec = P(("rep", "data"), None)
    id_spec = P(("rep", "data"))
    owned_spec = P("data", None, None)

    def device_step(x, adapter_id, w_gate, w_up, w_down, a_gate, b_gate, a_up, b_up, a_down, b_down):
        tok, d = x.shape
        ff = w_gate.shape[1]
        per_owner, rank = a_gate.shape[:2]
        na = per_owner * rank
        cap = (3 * tok + groups - 1) // groups
        rows = groups * cap
        nq, nf, ra = d // KB, ff // KB, na // KB
        slots = 3 * 2 * (nf + ra)

        def flat(a):
            return a.reshape(-1, KB, a.shape[-1])

        hbm = pl.BlockSpec(memory_space=pl.ANY)
        vmem = pl.BlockSpec(memory_space=pltpu.VMEM)
        dma = pltpu.SemaphoreType.DMA
        return pl.pallas_call(
            functools.partial(kernel, groups, LORA_ALPHA / rank, rank),
            out_shape=jax.ShapeDtypeStruct((tok, d), BF16),
            in_specs=[hbm] * 11,
            out_specs=vmem,
            scratch_shapes=[
                pltpu.VMEM((1, tok), jnp.int32),
                pltpu.VMEM((tok, d), BF16),
                pltpu.VMEM((slots, KB, KB), BF16),
                pltpu.VMEM((2, nf, rows, KB), F32),
                pltpu.VMEM((2, ra, KB, rows), F32),
                pltpu.VMEM((ra, KB, rows), F32),
                pltpu.VMEM((2, ra, rows, KB), BF16),
                pltpu.VMEM((nq, rows, KB), BF16),
                pltpu.VMEM((nf, rows, KB), BF16),
                pltpu.VMEM((nq, groups, cap, KB), BF16),
                pltpu.VMEM((nq, groups, cap, KB), BF16),
                pltpu.VMEM((groups, cap, 128), BF16),
                pltpu.VMEM((groups, cap, 128), BF16),
                pltpu.VMEM((nq, groups, cap, KB), BF16),
                pltpu.VMEM((nq, groups, cap, KB), BF16),
                dma((3,)), dma((slots,)), dma((2,)),
                dma((nq, groups)), dma((nq, groups)),
                dma((groups,)), dma((groups,)),
                dma((nq, groups)), dma((nq, groups)),
            ],
            compiler_params=pltpu.CompilerParams(collective_id=0, has_side_effects=True, vmem_limit_bytes=VMEM_LIMIT),
            name="lora_layer",
        )(adapter_id.reshape(1, tok), x, w_gate, w_up, flat(w_down), flat(a_gate), flat(a_up), flat(a_down), flat(b_gate), flat(b_up), flat(b_down))

    return jax.shard_map(device_step, mesh=mesh, in_specs=(row_spec, id_spec, P(), P(), P(), owned_spec, owned_spec, owned_spec, owned_spec, owned_spec, owned_spec), out_specs=row_spec, check_vma=False)
```

```python
import functools

import jax
import jax.numpy as jnp
from jax import lax
from jax.experimental import pallas as pl
from jax.experimental.pallas import tpu as pltpu
from jax.sharding import PartitionSpec as P

LORA_ALPHA = 32
F32 = jnp.float32
BF16 = jnp.bfloat16
MESH = pl.DeviceIdType.MESH

KB = 512
VMEM_LIMIT = 67043328


def nt_dot(a, b):
    return lax.dot_general(a, b, (((1,), (1,)), ((), ())), preferred_element_type=F32)


def kernel(groups, scale, rank, ids_hbm, x_hbm, wg, wu, wd, ag, au, ad, bg, bu, bd, out_ref,
           ids_ref, x_ref, pool, acc, low, lowd, lowm, xs, hid, xsend, xrecv, lsend, lrecv, osend, orecv,
           w_sem, g_sem, in_sem, xs_sem, xr_sem, ls_sem, lr_sem, os_sem, or_sem):
    me = lax.axis_index("data")
    partner = me + 1 - 2 * lax.rem(me, 2)
    tok, d = x_hbm.shape
    nf, ra = wd.shape[0], ag.shape[0]
    na = ra * KB
    per_owner = na // rank
    cap = xsend.shape[2]
    rows = groups * cap
    slots = pool.shape[0]
    nq = nm = d // KB

    peers = [lax.rem(base + 4, groups) for base in (me, partner)]
    peers += [lax.rem(me + 2, groups), lax.rem(me + 6, groups), lax.rem(partner + 2, groups), lax.rem(partner + 6, groups), partner]
    assert groups == 8
    links = range(groups - 1)

    barrier = pltpu.get_barrier_semaphore()
    for to in peers:
        pl.semaphore_signal(barrier, inc=1, device_id={"data": to}, device_id_type=MESH)
    ids_copy = pltpu.make_async_copy(ids_hbm, ids_ref, in_sem.at[0])
    x_in = pltpu.make_async_copy(x_hbm, x_ref, in_sem.at[1])
    ids_copy.start()
    x_in.start()

    per_k = 2 * (nf + ra)
    per_f = 3 * ra
    per_m = nf + ra
    f_base = nq * per_k
    per_b = 2 * ra
    m_base = f_base + nf * per_f
    total = m_base + nm * per_m

    def slot_of(i):
        return i % slots if isinstance(i, int) else lax.rem(i, slots)

    ring = slots // per_k
    assert slots % per_k == 0

    def w_block(q, p, n):
        s = slot_of(q * per_k + p * nf + n)
        return pltpu.make_async_copy((wg, wu)[p].at[pl.ds(q * KB, KB), pl.ds(n * KB, KB)], pool.at[s], w_sem.at[q % ring if isinstance(q, int) else lax.rem(q, ring)])

    def w_wait(q):
        s = slot_of(q * per_k)
        every = pool.at[pl.ds(s, 2 * nf)]
        pltpu.make_async_copy(every, every, w_sem.at[q % ring if isinstance(q, int) else lax.rem(q, ring)]).wait()

    def group(src, c, i):
        count = src.shape[0]
        s = slot_of(i)
        if isinstance(s, int):
            assert s + count <= slots
        return pltpu.make_async_copy(src.at[:, :, pl.ds(c * KB, KB)], pool.at[pl.ds(s, count)], g_sem.at[s])

    def a_group(q, p):
        return group((ag, au)[p], q, q * per_k + 2 * nf + p * ra)

    def b_at(f, p):
        return f_base + (p * ra if isinstance(f, int) and f == 0 else f * per_f - ra + p * ra)

    def b_group(f, p):
        return group((bg, bu)[p], f, b_at(f, p))

    def ad_at(f):
        return m_base - ra if isinstance(f, int) and f == nf - 1 else f_base + (f + 1) * per_f + per_b - ra

    def ad_group(f):
        return group(ad, f, ad_at(f))

    def bd_group(m):
        return group(bd, m, m_base + m * per_m)

    def wd_group(m):
        return group(wd, m, m_base + m * per_m + ra)

    later = [(b_at(f, p), ra, b_group(f, p)) for f in range(nf) for p in range(2)]
    later += [(ad_at(f), ra, ad_group(f)) for f in range(nf)]
    later += [(m_base + m * per_m, ra, bd_group(m)) for m in range(nm)]
    later += [(m_base + m * per_m + ra, nf, wd_group(m)) for m in range(nm)]
    later.sort(key=lambda t: t[0])
    assert [t[0] for t in later] == [f_base + sum(t[1] for t in later[:k]) for k in range(len(later))]

    def k_start(q):
        for p in range(2):
            for n in range(nf):
                w_block(q, p, n).start(priority=1)
            a_group(q, p).start(priority=1)

    def start_between(lo, hi):
        for i, count, copy in later:
            if lo <= i + count - 1 - slots < hi:
                copy.start(priority=1)

    k_start(0)

    ids_copy.wait()
    ids_row = ids_ref[...]
    own_row = ids_row // per_owner
    ti = lax.broadcasted_iota(jnp.int32, (tok, tok), 0)
    tj = lax.broadcasted_iota(jnp.int32, (tok, tok), 1)
    eye = ti == tj
    ids_col = jnp.sum(jnp.where(eye, ids_row, 0), axis=1, keepdims=True)
    own_col = ids_col // per_owner
    same = own_col == own_row
    arr_row = jnp.sum(jnp.where(jnp.logical_and(same, ti < tj), 1, 0), axis=0, keepdims=True)
    arr_col = jnp.sum(jnp.where(jnp.logical_and(same, tj < ti), 1, 0), axis=1, keepdims=True)
    slot_row = own_row * cap + arr_row
    slot_col = own_col * cap + arr_col
    pick = (lax.broadcasted_iota(jnp.int32, (rows, tok), 0) == slot_row).astype(F32).astype(BF16)
    back = (lax.broadcasted_iota(jnp.int32, (tok, rows), 1) == slot_col).astype(F32).astype(BF16)
    loc = jnp.broadcast_to((ids_col - own_col * per_owner).astype(F32), (tok, 128)).astype(BF16)
    lsend[...] = jnp.dot(pick, loc, preferred_element_type=F32).reshape(groups, cap, 128).astype(BF16)
    x_in.wait()
    for q in range(nq):
        part = jnp.dot(pick, x_ref[:, q * KB:(q + 1) * KB], preferred_element_type=F32)
        xsend[q] = part.reshape(groups, cap, KB).astype(BF16)

    pl.semaphore_wait(barrier, groups - 1)

    def remote(src, dst, j, send_sem, recv_sem):
        return pltpu.make_async_remote_copy(src.at[peers[j]], dst.at[me], send_sem.at[j], recv_sem.at[j], device_id={"data": peers[j]}, device_id_type=MESH)

    def l_copy(j):
        return remote(lsend, lrecv, j, ls_sem, lr_sem)

    def x_copy(q, j):
        return remote(xsend.at[q], xrecv.at[q], j, xs_sem.at[q], xr_sem.at[q])

    def o_copy(m, j):
        return remote(osend.at[m], orecv.at[m], j, os_sem.at[m], or_sem.at[m])

    for q in range(nq):
        for j in links:
            x_copy(q, j).start()
    for j in links:
        l_copy(j).start()
    for q in range(1, ring):
        k_start(q)
    lrecv[me] = lsend[me]
    for q in range(nq):
        xrecv[q, me] = xsend[q, me]

    low[...] = jnp.zeros_like(low)
    acc[...] = jnp.zeros_like(acc)
    lowd[...] = jnp.zeros_like(lowd)

    def k_in(q):
        for j in links:
            x_copy(q, j).wait_recv()
        xq = xrecv[q].astype(F32).reshape(rows, KB).astype(BF16)
        xs[q] = xq
        for p in range(2):
            a_group(q, p).wait()
        w_wait(q)
        return xq

    def k_low(q, xq):
        for p in range(2):
            for r in range(ra):
                low[p, r] += nt_dot(pool[slot_of(q * per_k + 2 * nf + p * ra) + r], xq)

    def k_base(q, xq, lo, hi):
        s0 = slot_of(q * per_k)
        for p in range(2):
            for n in range(lo, hi):
                acc[p, n] += jnp.dot(xq, pool[s0 + p * nf + n], preferred_element_type=F32)

    def k_step(q, carry):
        xq = k_in(q)
        k_low(q, xq)
        k_base(q, xq, 0, nf)
        for z in range(nq - 1):
            @pl.when(q == z)
            def _():
                if z + ring < nq:
                    k_start(z + ring)
                start_between(z * per_k, (z + 1) * per_k)
        return carry

    lax.fori_loop(0, nq - 1, k_step, 0)

    def low_dot(p, i0):
        full = jnp.dot(lowm[p, 0], pool[slot_of(i0)], preferred_element_type=F32)
        for r in range(1, ra):
            full += jnp.dot(lowm[p, r], pool[slot_of(i0) + r], preferred_element_type=F32)
        return (scale * full).astype(BF16).astype(F32)

    def hidden(f):
        g = acc[0, f] + low_dot(0, b_at(f, 0))
        u = acc[1, f] + low_dot(1, b_at(f, 1))
        return (jax.nn.silu(g) * u).astype(BF16)

    xq = k_in(nq - 1)
    for p in range(2):
        b_group(0, p).wait()
    for j in links:
        l_copy(j).wait_recv()
    loc_in = lrecv[...].astype(F32).reshape(rows, 128).astype(BF16)
    lane0 = (lax.broadcasted_iota(jnp.int32, (8, 128), 1) == 0).astype(F32).astype(BF16)
    loc_row = nt_dot(lane0, loc_in)[0:1, :]
    ad_col = (lax.broadcasted_iota(jnp.int32, (KB, rows), 0) // rank).astype(F32)
    unit = (lax.broadcasted_iota(jnp.int32, (rows, rows), 0) == lax.broadcasted_iota(jnp.int32, (rows, rows), 1)).astype(F32).astype(BF16)

    def keep_own(v, r):
        own = ad_col + float(r * (KB // rank)) == loc_row
        kept = jnp.where(own, v, 0.0).astype(BF16)
        return nt_dot(unit, kept).astype(BF16)

    k_low(nq - 1, xq)
    k_base(nq - 1, xq, 0, nf // 3)
    for p in range(2):
        for r in range(ra):
            lowm[p, r] = keep_own(low[p, r], r)
    k_base(nq - 1, xq, nf // 3, 2 * nf // 3)
    hid[0] = hidden(0)
    k_base(nq - 1, xq, 2 * nf // 3, nf)
    start_between((nq - 1) * per_k, f_base + per_b)
    for j in links:
        l_copy(j).wait_send()
        for q in range(nq):
            x_copy(q, j).wait_send()

    def low_down(f):
        for r in range(ra):
            lowd[r] += nt_dot(pool[slot_of(ad_at(f)) + r], hid[f])

    def f_step(g, carry):
        steps = [pair * g + 1 + z for z in range(pair)]
        for f in steps:
            for p in range(2):
                b_group(f, p).wait()
            ad_group(f - 1).wait()
        for f in steps:
            h = hidden(f)
            low_down(f - 1)
            hid[f] = h
        for z in range((nf - 1) // pair):
            @pl.when(g == z)
            def _():
                lo = f_base + per_b + z * pair * per_f
                start_between(lo, lo + pair * per_f)
        return carry

    pair = 2 if nf % 2 == 1 else 1
    lax.fori_loop(0, (nf - 1) // pair, f_step, 0)
    assert m_base - ra + slots >= total

    def m_in(m):
        bd_group(m).wait()
        wd_group(m).wait()

    def m_base_dot(m):
        s0 = slot_of(m_base + m * per_m + ra)
        base = jnp.dot(hid[0], pool[s0], preferred_element_type=F32)
        for k in range(1, nf):
            base += jnp.dot(hid[k], pool[s0 + k], preferred_element_type=F32)
        return base

    def m_out(m, base):
        res = xs[m].astype(F32) + (base + low_dot(0, m_base + m * per_m))
        osend[m] = res.reshape(groups, cap, KB).astype(BF16)
        for j in links:
            o_copy(m, j).start()
        orecv[m, me] = osend[m, me]

    ad_group(nf - 1).wait()
    m_in(0)
    low_down(nf - 1)
    base = m_base_dot(0)
    for r in range(ra):
        lowm[0, r] = keep_own(lowd[r], r)
    m_out(0, base)

    def m_step(m, carry):
        m_in(m)
        m_out(m, m_base_dot(m))
        return carry

    lax.fori_loop(1, nm, m_step, 0)

    for m in range(nm):
        for j in links:
            o_copy(m, j).wait_recv()
            o_copy(m, j).wait_send()
        got = orecv[m].astype(F32).reshape(rows, KB).astype(BF16)
        out_ref[:, m * KB:(m + 1) * KB] = jnp.dot(back, got, preferred_element_type=F32).astype(BF16)


def solution(mesh):
    groups = mesh.shape["data"]
    row_spec = P(("rep", "data"), None)
    id_spec = P(("rep", "data"))
    owned_spec = P("data", None, None)

    def device_step(x, adapter_id, w_gate, w_up, w_down, a_gate, b_gate, a_up, b_up, a_down, b_down):
        tok, d = x.shape
        ff = w_gate.shape[1]
        per_owner, rank = a_gate.shape[:2]
        na = per_owner * rank
        cap = (3 * tok + groups - 1) // groups
        rows = groups * cap
        nq, nf, ra = d // KB, ff // KB, na // KB
        slots = 3 * 2 * (nf + ra)

        def flat(a):
            return a.reshape(-1, KB, a.shape[-1])

        hbm = pl.BlockSpec(memory_space=pl.ANY)
        vmem = pl.BlockSpec(memory_space=pltpu.VMEM)
        dma = pltpu.SemaphoreType.DMA
        return pl.pallas_call(
            functools.partial(kernel, groups, LORA_ALPHA / rank, rank),
            out_shape=jax.ShapeDtypeStruct((tok, d), BF16),
            in_specs=[hbm] * 11,
            out_specs=vmem,
            scratch_shapes=[
                pltpu.VMEM((1, tok), jnp.int32),
                pltpu.VMEM((tok, d), BF16),
                pltpu.VMEM((slots, KB, KB), BF16),
                pltpu.VMEM((2, nf, rows, KB), F32),
                pltpu.VMEM((2, ra, KB, rows), F32),
                pltpu.VMEM((ra, KB, rows), F32),
                pltpu.VMEM((2, ra, rows, KB), BF16),
                pltpu.VMEM((nq, rows, KB), BF16),
                pltpu.VMEM((nf, rows, KB), BF16),
                pltpu.VMEM((nq, groups, cap, KB), BF16),
                pltpu.VMEM((nq, groups, cap, KB), BF16),
                pltpu.VMEM((groups, cap, 128), BF16),
                pltpu.VMEM((groups, cap, 128), BF16),
                pltpu.VMEM((nq, groups, cap, KB), BF16),
                pltpu.VMEM((nq, groups, cap, KB), BF16),
                dma((3,)), dma((slots,)), dma((2,)),
                dma((nq, groups)), dma((nq, groups)),
                dma((groups,)), dma((groups,)),
                dma((nq, groups)), dma((nq, groups)),
            ],
            compiler_params=pltpu.CompilerParams(collective_id=0, has_side_effects=True, vmem_limit_bytes=VMEM_LIMIT),
            name="lora_layer",
        )(adapter_id.reshape(1, tok), x, w_gate, w_up, flat(w_down), flat(a_gate), flat(a_up), flat(a_down), flat(b_gate), flat(b_up), flat(b_down))

    return jax.shard_map(device_step, mesh=mesh, in_specs=(row_spec, id_spec, P(), P(), P(), owned_spec, owned_spec, owned_spec, owned_spec, owned_spec, owned_spec), out_specs=row_spec, check_vma=False)
```
